32 devices in a mesh: row: 8 (over z, x), col: 4 (over y, core).
Axes of the slice: x: 2, y: 2, z: 4, core: 2. Of those that a mesh axis runs over, the one named last changes fastest.
Arguments:
- eigvecs: float32 [16384, 4096], P('row', 'col'), may hold values from -6 to 6
- reflectors: float32 [2, 16384, 256], P(None, ('row', 'col')), may hold values from -0.13258252 to 0.13258252
- tfactors: float32 [2, 256, 256], replicated, may hold values from -1 to 2, as said below
Outputs:
- back: float32 [16384, 4096], P('row', 'col')
The draws below stay inside these ranges and needn't reach their ends.
Inputs may be any that keep to these rules, and one draw needn't show every extreme that they name: Each tfactors[p] is upper triangular; its diagonal lies between 0.3 and 1.9.
All inputs are finite; a program needn't handle non-finite values.
Results may differ from the reference program's by a relative error of at most 0.00014.
Values sent between devices are 32-bit elements; how exact they have to be, the bound alone decides.
No kernel may reach another device: no remote copies, remote signals or barrier semaphores. Data moves between devices by JAX's collectives and lax.ppermute only.
A program may use at most 128 MiB of HBM per device.

```python
import jax
import jax.numpy as jnp
from jax import lax

NB = 256
PANELS = 2
N = 16384
K = 4096


def draw_tfactors(key, part):
    first = jax.random.fold_in(key, 11)
    second = jax.random.fold_in(key, 12)
    offdiag = jnp.clip(jax.random.normal(first, (PANELS, NB, NB), jnp.float32), -3.0, 3.0) / jnp.sqrt(jnp.float32(NB))
    diagonal = jax.random.uniform(second, (PANELS, NB), jnp.float32, 0.5, 1.5)
    upper_part = jnp.triu(offdiag, 1)
    eye_mat = jnp.eye(NB, dtype=jnp.float32)
    return (upper_part + eye_mat[None, :, :] * diagonal[:, None, :]).astype(jnp.float32)


def steps_of(rng, shape, cuts, smallest, top_value):
    def one(axis_at, blocks):
        draws = jax.random.uniform(jax.random.fold_in(jax.random.fold_in(rng, 6), axis_at), (blocks,), jnp.float32, smallest / len(cuts), top_value / len(cuts))
        return jnp.repeat(jnp.exp(draws), shape[axis_at] // blocks).reshape((-1,) + (1,) * (len(shape) - axis_at - 1))

    loudness = one(*cuts[0])
    for cut in cuts[1:]:
        loudness = loudness * one(*cut)
    return loudness


def gaussian(rng, dims, spread, bound, cuts=(), kind=jnp.bfloat16):
    loudness = steps_of(rng, dims, cuts, -0.22, 0.18) if cuts else 1.0
    drawn = jax.random.normal(rng, dims, jnp.float32) * spread * loudness
    return jnp.minimum(jnp.maximum(drawn, -bound), bound).astype(kind)


def setup_inputs(seed: int = 0) -> dict:
    seeds = jax.random.split(jax.random.key(seed), 4)
    eigvecs = gaussian(seeds[0], (N, K), 1.0, 6.0, ((0, 8), (1, 4)), jnp.float32)
    reflectors = gaussian(seeds[1], (PANELS, N, NB), ((N * NB) ** -0.25), 0.13258252, ((1, 32),), jnp.float32)
    tfactors = draw_tfactors(jax.random.fold_in(seeds[3], 71), 0)
    return {"eigvecs": eigvecs, "reflectors": reflectors, "tfactors": tfactors}


def product(left, right):
    return jnp.dot(left, right, precision=lax.Precision.HIGHEST, preferred_element_type=jnp.float32)


def reference(eigvecs, reflectors, tfactors):
    current = eigvecs
    for panel_idx in range(PANELS - 1, -1, -1):
        block = reflectors[panel_idx]
        inner_prod = product(block.T, current)
        coeffs = product(tfactors[panel_idx], inner_prod)
        current = current - product(block, coeffs)
    return current
```

```python
import functools

import jax
import jax.numpy as jnp
from jax import lax
from jax.experimental import pallas as pl
from jax.experimental.pallas import tpu as pltpu
from jax.sharding import PartitionSpec as P

LANES = 128
NN = (((1,), (0,)), ((), ()))
NT = (((1,), (1,)), ((), ()))
TN = (((0,), (0,)), ((), ()))


def exchange(value, axis, size, bit):
    return lax.ppermute(value, axis, [(i, i ^ bit) for i in range(size)])


def split(value):
    high = value.astype(jnp.bfloat16)
    low = (value - high.astype(jnp.float32)).astype(jnp.bfloat16)
    return high, low


def dot(left, right, dims):
    return lax.dot_general(left, right, dims, preferred_element_type=jnp.float32)


def dot3(left_high, left_low, right_high, right_low, dims):
    return (
        dot(left_high, right_high, dims)
        + dot(left_high, right_low, dims)
        + dot(left_low, right_high, dims)
    )


def exact(left, right, dims):
    return lax.dot_general(
        left, right, dims, precision=lax.Precision.HIGHEST, preferred_element_type=jnp.float32
    )


def bit_reverse(index, bits):
    out = 0
    for b in range(bits):
        out |= ((index >> b) & 1) << (bits - 1 - b)
    return out


def column_block(me, position, bits):
    return lax.bitwise_xor(me, jnp.int32(bit_reverse(position, bits)))


def params(*semantics):
    return pltpu.CompilerParams(dimension_semantics=semantics, vmem_limit_bytes=56 * 2**20)


def cost(flops, moved):
    return pl.CostEstimate(flops=int(flops), bytes_accessed=int(moved), transcendentals=0)


def whole(shape):
    return pl.BlockSpec(shape, lambda *_: (0,) * len(shape))


def prepare_body(bits, ids, e_ref, high_ref, low_ref):
    count = 1 << bits
    wide = e_ref.shape[1] // count
    for position in range(count):
        at = pl.multiple_of(column_block(ids[0], position, bits) * wide, wide)
        turned = e_ref[:, pl.ds(at, wide)].T
        high, low = split(turned)
        high_ref[position * wide : (position + 1) * wide, :] = high
        low_ref[position * wide : (position + 1) * wide, :] = low


def prepare(ids, eigvecs, parts, bits):
    rows, cols = eigvecs.shape
    step = rows // parts
    out = jax.ShapeDtypeStruct((cols, rows), jnp.bfloat16)
    spec = pl.BlockSpec((cols, step), lambda k, ids: (0, k))
    return pl.pallas_call(
        functools.partial(prepare_body, bits),
        grid_spec=pltpu.PrefetchScalarGridSpec(
            num_scalar_prefetch=1,
            grid=(parts,),
            in_specs=[pl.BlockSpec((step, cols), lambda k, ids: (lax.bitwise_xor(ids[1], k), 0))],
            out_specs=[spec, spec],
        ),
        out_shape=[out, out],
        compiler_params=params("arbitrary"),
        cost_estimate=cost(rows * cols * 2000, rows * cols * 8),
        name="prepare",
    )(ids, eigvecs)


def gram_body(v_ref, out_ref):
    upper_high, upper_low = split(v_ref[1])
    lower_high, lower_low = split(v_ref[0])
    out_ref[...] = dot3(upper_high, upper_low, lower_high, lower_low, TN)


def gram(shard):
    _, rows, nb = shard.shape
    return pl.pallas_call(
        gram_body,
        grid=(1,),
        in_specs=[whole(shard.shape)],
        out_specs=whole((nb, nb)),
        out_shape=jax.ShapeDtypeStruct((nb, nb), jnp.float32),
        compiler_params=params("arbitrary"),
        cost_estimate=cost(6 * rows * nb * nb, 8 * rows * nb),
        name="gram",
    )(shard)


def near_body(count, high_ref, low_ref, *refs):
    shards = refs[:count]
    outs = refs[count : count + 2]
    v_high, v_low = refs[count + 2 :]
    depth = shards[0].shape[1]

    @pl.when(pl.program_id(0) == 0)
    def _():
        for panel in range(2):
            for k, ref in enumerate(shards):
                high, low = split(ref[panel])
                v_high[panel, k * depth : (k + 1) * depth, :] = high
                v_low[panel, k * depth : (k + 1) * depth, :] = low

    for panel in range(2):
        outs[panel][...] = dot3(high_ref[...], low_ref[...], v_high[panel], v_low[panel], NN)


def near_products(e_high, e_low, shards):
    cols = e_high.shape[0]
    _, depth, nb = shards[0].shape
    deep = depth * len(shards)
    tile = cols // 4
    e_spec = pl.BlockSpec((tile, deep), lambda m: (m, 0))
    out = jax.ShapeDtypeStruct((cols, nb), jnp.float32)
    out_spec = pl.BlockSpec((tile, nb), lambda m: (m, 0))
    return pl.pallas_call(
        functools.partial(near_body, len(shards)),
        grid=(4,),
        in_specs=[e_spec, e_spec] + [whole(s.shape) for s in shards],
        out_specs=[out_spec, out_spec],
        out_shape=[out, out],
        scratch_shapes=[pltpu.VMEM((2, deep, nb), jnp.bfloat16)] * 2,
        compiler_params=params("arbitrary"),
        cost_estimate=cost(12 * cols * deep * nb, 4 * cols * deep),
        name="near_products",
    )(e_high, e_low, *shards)


def far_body(count, high_ref, low_ref, base_ref, *refs):
    shards = refs[:count]
    keep_ref, send_ref, v_high, v_low = refs[count:]
    depth = shards[0].shape[0]
    m = pl.program_id(0)

    @pl.when(m == 0)
    def _():
        for k, ref in enumerate(shards):
            high, low = split(ref[...])
            v_high[k * depth : (k + 1) * depth, :] = high
            v_low[k * depth : (k + 1) * depth, :] = low

    total = base_ref[...] + dot3(high_ref[...], low_ref[...], v_high[...], v_low[...], NN)

    @pl.when(m < 2)
    def _():
        send_ref[...] = total

    @pl.when(m >= 2)
    def _():
        keep_ref[...] = total


def far_products(e_high, e_low, base, shards):
    cols = e_high.shape[0]
    depth, nb = shards[0].shape
    deep = depth * len(shards)
    tile = cols // 4
    turn = lambda m: lax.rem(m + 2, 4)
    e_spec = pl.BlockSpec((tile, deep), lambda m: (turn(m), 1))
    out = jax.ShapeDtypeStruct((cols // 2, nb), jnp.float32)
    return pl.pallas_call(
        functools.partial(far_body, len(shards)),
        grid=(4,),
        in_specs=[e_spec, e_spec, pl.BlockSpec((tile, nb), lambda m: (turn(m), 0))]
        + [whole(s.shape) for s in shards],
        out_specs=[
            pl.BlockSpec((tile, nb), lambda m: (jnp.maximum(m - 2, 0), 0)),
            pl.BlockSpec((tile, nb), lambda m: (jnp.minimum(m, 1), 0)),
        ],
        out_shape=[out, out],
        scratch_shapes=[pltpu.VMEM((deep, nb), jnp.bfloat16)] * 2,
        compiler_params=params("arbitrary"),
        cost_estimate=cost(6 * cols * deep * nb, 4 * cols * deep),
        name="far_products",
    )(e_high, e_low, base, *shards)


def upper_body(keep_ref, got_ref, t_ref, out_ref):
    out_ref[...] = exact(keep_ref[...] + got_ref[...], t_ref[1], NT)


def upper_coeffs(keep, got, tfactors):
    rows, nb = keep.shape
    return pl.pallas_call(
        upper_body,
        grid=(1,),
        in_specs=[whole(keep.shape), whole(got.shape), whole(tfactors.shape)],
        out_specs=whole(keep.shape),
        out_shape=jax.ShapeDtypeStruct(keep.shape, jnp.float32),
        compiler_params=params("arbitrary"),
        cost_estimate=cost(12 * rows * nb * nb, 12 * rows * nb),
        name="upper_coeffs",
    )(keep, got, tfactors)


def lower_body(ids, keep_ref, got_ref, upper_ref, g_own, g_got, t_ref, out_ref):
    half = g_own.shape[0]
    flipped = lax.bitwise_and(ids[0], 1) == 1
    first = jnp.where(flipped, g_got[...], g_own[...])
    second = jnp.where(flipped, g_own[...], g_got[...])
    cross = exact(upper_ref[:, :half], first, NN) + exact(upper_ref[:, half:], second, NN)
    out_ref[...] = exact(keep_ref[...] + got_ref[...] - cross, t_ref[0], NT)


def lower_coeffs(ids, keep, got, upper, g_own, g_got, tfactors):
    rows, nb = keep.shape
    args = (keep, got, upper, g_own, g_got, tfactors)
    return pl.pallas_call(
        lower_body,
        grid_spec=pltpu.PrefetchScalarGridSpec(
            num_scalar_prefetch=1,
            grid=(1,),
            in_specs=[whole(a.shape) for a in args],
            out_specs=whole(keep.shape),
        ),
        out_shape=jax.ShapeDtypeStruct(keep.shape, jnp.float32),
        compiler_params=params("arbitrary"),
        cost_estimate=cost(24 * rows * nb * nb, 12 * rows * nb),
        name="lower_coeffs",
    )(ids, *args)


def update_body(bits, count, ids, e_ref, c_own, c_got, *refs):
    shards = refs[:count]
    out_ref, c_high, c_low, v_high, v_low = refs[count:]
    k, sub = pl.program_id(0), pl.program_id(1)
    half = c_own.shape[0]
    blocks = 1 << bits
    wide = 2 * half // blocks

    @pl.when((k == 0) & (sub == 0))
    def _():
        for at, ref in ((0, c_own), (half, c_got)):
            high, low = split(ref[...])
            c_high[at : at + half, :] = high
            c_low[at : at + half, :] = low

    for i, ref in enumerate(shards):

        @pl.when((k == i) & (sub == 0))
        def _(ref=ref):
            high, low = split(ref[...])
            v_high[...] = high
            v_low[...] = low

    rows = out_ref.shape[0]
    here = pl.ds(pl.multiple_of(sub * rows, rows), rows)
    left_high, left_low = v_high[here, :], v_low[here, :]
    for pair in range(blocks // 2):
        span = slice(2 * pair * wide, (2 * pair + 2) * wide)
        part = dot3(left_high, left_low, c_high[span, :], c_low[span, :], NT)
        for j in range(2):
            at = pl.multiple_of(column_block(ids[0], 2 * pair + j, bits) * wide, wide)
            cut = pl.ds(at, wide)
            out_ref[:, cut] = e_ref[:, cut] - part[:, j * wide : (j + 1) * wide]


def update(ids, current, c_own, c_got, shards, bits):
    rows, cols = current.shape
    depth, nb = shards[0].shape
    subs = 2
    spec = pl.BlockSpec(
        (depth // subs, cols), lambda k, s, ids: (lax.bitwise_xor(ids[1], k) * subs + s, 0)
    )
    return pl.pallas_call(
        functools.partial(update_body, bits, len(shards)),
        grid_spec=pltpu.PrefetchScalarGridSpec(
            num_scalar_prefetch=1,
            grid=(len(shards), subs),
            in_specs=[spec, whole(c_own.shape), whole(c_got.shape)]
            + [whole(s.shape) for s in shards],
            out_specs=spec,
            scratch_shapes=[pltpu.VMEM((cols, nb), jnp.bfloat16)] * 2
            + [pltpu.VMEM((depth, nb), jnp.bfloat16)] * 2,
        ),
        out_shape=jax.ShapeDtypeStruct(current.shape, jnp.float32),
        compiler_params=params("arbitrary", "arbitrary"),
        cost_estimate=cost(6 * rows * cols * nb, 8 * rows * cols),
        name="update",
    )(ids, current, c_own, c_got, *shards)


def local(row_size, col_size, eigvecs, reflectors, tfactors):
    cols = eigvecs.shape[1]
    row_bits = row_size.bit_length() - 1
    bits = min(row_bits, (cols // LANES).bit_length() - 1)
    half_parts = col_size // 2
    me = lax.axis_index("row")
    ids = jnp.stack(
        [lax.bitwise_and(me, (1 << bits) - 1), lax.axis_index("col")]
    ).astype(jnp.int32)

    def spread(found, top):
        bit = top
        while bit:
            for k in sorted(found):
                found[k ^ bit] = exchange(found[k], "col", col_size, bit)
            bit >>= 1
        return found

    far = []
    for panel in (1, 0):
        far.append(exchange(reflectors[panel], "col", col_size, half_parts))
    near = spread({0: reflectors}, half_parts // 2)
    near = [near[k] for k in range(half_parts)]

    own_gram = gram(reflectors)
    e_high, e_low = prepare(ids, eigvecs, col_size, bits)

    flip = lax.bitwise_and(me, 1)
    g_half = own_gram.shape[0] // 2
    g_send = lax.dynamic_slice_in_dim(own_gram, (1 - flip) * g_half, g_half, 0)
    g_own = lax.dynamic_slice_in_dim(own_gram, flip * g_half, g_half, 0)
    g_own = g_own + exchange(g_send, "row", row_size, 1)
    for b in range(1, row_bits):
        g_own = g_own + exchange(g_own, "row", row_size, 1 << b)
    for b in range(col_size.bit_length() - 1):
        g_own = g_own + exchange(g_own, "col", col_size, 1 << b)
    g_got = exchange(g_own, "row", row_size, 1)

    near_upper_lower = near_products(e_high, e_low, near)

    coeffs = None
    current = eigvecs
    panel_shards, pieces = {}, {}
    for panel, sent in ((1, far[0]), (0, far[1])):
        got = spread({0: sent}, half_parts // 2)
        got = [got[k] for k in range(half_parts)]
        panel_shards[panel] = [s[panel] for s in near] + got
        keep, send = far_products(e_high, e_low, near_upper_lower[panel], got)
        came = exchange(send, "row", row_size, 1)
        for b in range(1, bits):
            half = keep.shape[0] // 2
            send = keep[half:] + came[half:]
            keep = keep[:half] + came[:half]
            came = exchange(send, "row", row_size, 1 << b)
        for b in range(bits, row_bits):
            keep = keep + came
            came = exchange(keep, "row", row_size, 1 << b)
        pieces[panel] = (keep, came)

    for panel in (1, 0):
        keep, came = pieces[panel]
        if panel == 1:
            coeffs = upper_coeffs(keep, came, tfactors)
        else:
            coeffs = lower_coeffs(ids, keep, came, coeffs, g_own, g_got, tfactors)
        found = coeffs
        for b in range(bits - 1, 0, -1):
            found = jnp.concatenate([found, exchange(found, "row", row_size, 1 << b)], 0)
        other = exchange(found, "row", row_size, 1)
        current = update(ids, current, found, other, panel_shards[panel], bits)
    return current


def solution(mesh):
    return jax.shard_map(
        functools.partial(local, mesh.shape["row"], mesh.shape["col"]),
        mesh=mesh,
        in_specs=(P("row", "col"), P(None, ("row", "col"), None), P()),
        out_specs=P("row", "col"),
        check_vma=False,
    )
```
